32 devices in a mesh: inst: 4 (over y, core), cells: 8 (over z, x).
Axes of the slice: x: 2, y: 2, z: 4, core: 2. Of those that a mesh axis runs over, the one named last changes fastest.
Arguments:
- flow_state: float32 [8, 5, 64, 32, 128], P('inst', None, 'cells'), may hold values from -6 to 6
- forcing: float32 [8, 5, 64, 32, 128], P('inst', None, 'cells'), may hold values from -6 to 6
- diffusion: float32 [64, 32, 128], P('cells'), may hold values from 0.2 to 0.6
- block_inverse: float32 [5, 5, 64, 32, 128], P(None, None, 'cells', 'inst'), may hold values from -0.03 to 0.15, as said below
Outputs:
- new_state: float32 [8, 5, 64, 32, 128], P('inst', None, 'cells')
The draws below stay inside these ranges and needn't reach their ends.
Inputs may be any that keep to these rules, and one draw needn't show every extreme that they name: block_inverse[v, v] lies between 0.06 and 0.15; entries off the diagonal lie between -0.03 and 0.03.
All inputs are finite; a program needn't handle non-finite values.
Results may differ from the reference program's by a relative error of at most 0.0001.
Values sent between devices are 32-bit elements; how exact they have to be, the bound alone decides.
A program may use at most 64 MiB of HBM per device.

```python
import math
import jax
import jax.numpy as jnp
from jax import lax

INSTANCES = 8
VARIABLES = 5
NZ = 128
SWEEPS = 4
NX = 64
NY = 32


def draw_block_inverse(key, part):
    first_key, second_key = jax.random.split(jax.random.fold_in(key, 17))
    shape = (VARIABLES, VARIABLES, NX, NY, NZ)
    diagonal_vals = 0.06 * jnp.exp(jax.random.uniform(first_key, shape) * math.log(2.5))
    off_vals = jnp.clip(0.012 * jax.random.normal(second_key, shape), -0.03, 0.03)
    identity = jnp.eye(VARIABLES)[:, :, None, None, None]
    return jnp.where(identity > 0.5, diagonal_vals, off_vals).astype(jnp.float32)


def block_levels(key, shape, cuts, smallest, top_value):
    def one(dim, parts):
        steps = jax.random.uniform(jax.random.fold_in(jax.random.fold_in(key, 6), dim), (parts,), jnp.float32, smallest / len(cuts), top_value / len(cuts))
        return jnp.repeat(jnp.exp(steps), shape[dim] // parts).reshape((-1,) + (1,) * (len(shape) - dim - 1))

    loudness = one(*cuts[0])
    for cut in cuts[1:]:
        loudness = loudness * one(*cut)
    return loudness


def noise(own_key, dims, spread, most, cuts=(), held_as=jnp.bfloat16):
    values = jax.random.normal(own_key, dims, jnp.float32) * spread
    if len(cuts) > 0:
        values = block_levels(own_key, dims, cuts, -0.22, 0.18) * values
    return jnp.clip(values, min=-most, max=most).astype(held_as)


def setup_inputs(seed: int = 0) -> dict:
    arg_keys = jax.random.split(jax.random.key(seed), 5)
    return {
        "flow_state": noise(arg_keys[0], (INSTANCES, VARIABLES, NX, NY, NZ), 1.0, 6.0, ((0, 4), (2, 8)), jnp.float32),
        "forcing": noise(arg_keys[1], (INSTANCES, VARIABLES, NX, NY, NZ), 1.0, 6.0, ((0, 4), (2, 8)), jnp.float32),
        "diffusion": jnp.clip(jnp.exp(math.log(0.6) - 1.0986123 * jax.random.uniform(arg_keys[2], (NX, NY, NZ), jnp.float32) ** block_levels(arg_keys[2], (NX, NY, NZ), ((0, 8),), -0.2, 0.2)), 0.2, 0.6),
        "block_inverse": draw_block_inverse(jax.random.fold_in(arg_keys[4], 71), 0),
    }


frequency = 1.0


def spectral_matrix(count):
    index = jnp.arange(count)
    offset = index[:, None] - index[None, :]
    parity = jnp.where(offset % 2 == 0, 1.0, -1.0)
    angle = math.pi * jnp.where(offset == 0, 1, offset) / count
    entries = 0.5 * parity / jnp.tan(angle)
    return jnp.where(offset == 0, 0.0, entries).astype(jnp.float32)


def neighbour_sum(grid_field):
    padded = jnp.pad(grid_field, ((0, 0), (0, 0), (1, 1), (1, 1), (1, 1)))
    beside = padded[:, :, 2:, 1:-1, 1:-1] + padded[:, :, :-2, 1:-1, 1:-1]
    beside = beside + padded[:, :, 1:-1, 2:, 1:-1] + padded[:, :, 1:-1, :-2, 1:-1]
    beside = beside + padded[:, :, 1:-1, 1:-1, 2:] + padded[:, :, 1:-1, 1:-1, :-2]
    return beside


def spectral_term(matrix, grid_field):
    flat = grid_field.reshape(grid_field.shape[0], -1)
    product = jnp.dot(matrix, flat, precision=lax.Precision.HIGHEST)
    return (frequency * product).reshape(grid_field.shape)


def apply_blocks(block_inverse, source):
    return jnp.einsum("vwxyz,nwxyz->nvxyz", block_inverse, source, precision=lax.Precision.HIGHEST)


def reference(flow_state, forcing, diffusion, block_inverse):
    matrix = spectral_matrix(INSTANCES)
    weight = diffusion[None, None]
    residual = weight * (6.0 * flow_state - neighbour_sum(flow_state)) - forcing + spectral_term(matrix, flow_state)
    update = apply_blocks(block_inverse, -residual)
    for sweep_index in range(SWEEPS):
        source = -residual - spectral_term(matrix, update) + weight * neighbour_sum(update)
        update = apply_blocks(block_inverse, source)
    return flow_state + update
```

```python
import functools
import math

import jax
import jax.numpy as jnp
from jax import lax
from jax.experimental import pallas as pl
from jax.experimental.pallas import tpu as pltpu
from jax.sharding import PartitionSpec as P

SWEEPS = 4

frequency = 1.0

MESH = pl.DeviceIdType.MESH


def spectral_rows(values):
    count = len(values)
    differences, products = {}, {}

    def product(coefficient, low, high):
        if (low, high) not in differences:
            differences[low, high] = values[low] - values[high]
        if (coefficient, low, high) not in products:
            products[coefficient, low, high] = coefficient * differences[low, high]
        return products[coefficient, low, high]

    rows = []
    for n in range(count):
        total = None
        for k in range(1, (count + 1) // 2):
            coefficient = frequency * 0.5 * (-1.0) ** k / math.tan(math.pi * k / count)
            a, b = (n - k) % count, (n + k) % count
            if a > b:
                a, b, coefficient = b, a, -coefficient
            if coefficient < 0:
                term, sign = product(-coefficient, a, b), -1
            else:
                term, sign = product(coefficient, a, b), 1
            if total is None:
                total = term if sign > 0 else -term
            else:
                total = total + term if sign > 0 else total - term
        rows.append(total)
    return rows


def lane_sum(cur, lane):
    size = cur.shape[-1]
    left = jnp.where(lane == 0, 0.0, pltpu.roll(cur, 1, 1))
    right = jnp.where(lane == size - 1, 0.0, pltpu.roll(cur, size - 1, 1))
    return left + right


def kernel(inst_size, cells_size, state, forcing, diffusion, blocks, out,
           home, force, weight, block, part, state_blk, part_blk, residual, source, update,
           edge, halo, final, load_sem, own_sem, send_a, recv_a, send_b, recv_b, send_x, recv_x,
           send_u, recv_u, send_r, recv_r, send_o, recv_o):
    me, cell = lax.axis_index("inst"), lax.axis_index("cells")
    own, variables, planes, height, lanes = state.shape
    rows = height // inst_size
    count = own * inst_size

    def peer(step):
        return lax.rem(me + step, inst_size)

    def row_block(i):
        return pl.ds(pl.multiple_of(i * rows, rows), rows)

    has_before, has_after = cell > 0, cell < cells_size - 1
    has_above, has_below = me > 0, me < inst_size - 1
    before, after = {"cells": cell - 1}, {"cells": cell + 1}
    above, below = {"inst": me - 1}, {"inst": me + 1}

    def remote(src, dst, send, recv, target):
        return pltpu.make_async_remote_copy(
            src_ref=src, dst_ref=dst, send_sem=send, recv_sem=recv,
            device_id=target, device_id_type=MESH)

    loads = [
        pltpu.make_async_copy(state, home.at[:, :, pl.ds(1, planes)], load_sem.at[0]),
        pltpu.make_async_copy(forcing, force, load_sem.at[1]),
        pltpu.make_async_copy(diffusion, weight, load_sem.at[2]),
        pltpu.make_async_copy(
            state.at[:, :, :, row_block(me)], state_blk.at[pl.ds(me * own, own)], load_sem.at[3]),
        pltpu.make_async_copy(blocks, block, load_sem.at[4]),
    ]
    for load in loads:
        load.start()

    zero_home = jnp.zeros((own, variables, height, lanes), jnp.float32)

    @pl.when(jnp.logical_not(has_before))
    def _():
        home[:, :, 0] = zero_home

    @pl.when(jnp.logical_not(has_after))
    def _():
        home[:, :, planes + 1] = zero_home

    for s in range(SWEEPS):
        zero_blk = jnp.zeros((count, variables, rows, lanes), jnp.float32)

        @pl.when(jnp.logical_not(has_before))
        def _():
            update[s, :, :, 0] = zero_blk

        @pl.when(jnp.logical_not(has_after))
        def _():
            update[s, :, :, planes + 1] = zero_blk

        zero_halo = jnp.zeros((variables, planes, count, lanes), jnp.float32)

        @pl.when(jnp.logical_not(has_above))
        def _():
            halo[s, 0] = zero_halo

        @pl.when(jnp.logical_not(has_below))
        def _():
            halo[s, 1] = zero_halo

    barrier = pltpu.get_barrier_semaphore()
    for step in range(1, inst_size):
        pl.semaphore_signal(barrier, 1, device_id={"inst": peer(step)}, device_id_type=MESH)

    @pl.when(has_before)
    def _():
        pl.semaphore_signal(barrier, 1, device_id=before, device_id_type=MESH)

    @pl.when(has_after)
    def _():
        pl.semaphore_signal(barrier, 1, device_id=after, device_id_type=MESH)

    ends = jnp.where(has_before, 1, 0) + jnp.where(has_after, 1, 0)
    pl.semaphore_wait(barrier, inst_size - 1 + ends)

    to_before = remote(state.at[:, :, 0], home.at[:, :, planes + 1],
                       send_x.at[0], recv_x.at[1], before)
    to_after = remote(state.at[:, :, planes - 1], home.at[:, :, 0],
                      send_x.at[1], recv_x.at[0], after)
    pl.when(has_before)(to_before.start)
    pl.when(has_after)(to_after.start)

    moves = []
    for step in range(1, inst_size):
        moves.append(remote(
            state.at[:, :, :, row_block(peer(step))], state_blk.at[pl.ds(me * own, own)],
            send_a.at[step], recv_a.at[step], {"inst": peer(step)}))
        moves[-1].start()

    for load in loads[:3]:
        load.wait()
    lane = lax.broadcasted_iota(jnp.int32, (height, lanes), 1)
    row = lax.broadcasted_iota(jnp.int32, (height, lanes), 0)

    def local_plane(x):
        w = weight[x]
        for n in range(own):
            for v in range(variables):
                cur = home[n, v, x + 1]
                beside = home[n, v, x] + home[n, v, x + 2] + lane_sum(cur, lane)
                beside = beside + jnp.where(row == 0, 0.0, pltpu.roll(cur, 1, 0))
                beside = beside + jnp.where(row == height - 1, 0.0, pltpu.roll(cur, height - 1, 0))
                part[n, v, x] = w * (6.0 * cur - beside) - force[n, v, x]

    pl.loop(1, planes - 1)(local_plane)

    @pl.when(has_before)
    def _():
        to_after.wait_recv()

    @pl.when(has_after)
    def _():
        to_before.wait_recv()

    pl.loop(0, 2)(lambda i: local_plane(i * (planes - 1)))

    chunks = ((0, 1), (planes - 1, 1), (1, planes - 2))
    own_parts = pltpu.make_async_copy(
        part.at[:, :, :, row_block(me)], part_blk.at[pl.ds(me * own, own)], own_sem.at[0])
    own_parts.start()
    parts = [[] for _ in chunks]
    for c, (first, size) in enumerate(chunks):
        for step in range(1, inst_size):
            parts[c].append(remote(
                part.at[:, :, pl.ds(first, size), row_block(peer(step))],
                part_blk.at[pl.ds(me * own, own), :, pl.ds(first, size)],
                send_b.at[c, step], recv_b.at[c, step], {"inst": peer(step)}))
            parts[c][-1].start()

    loads[3].wait()
    loads[4].wait()
    own_parts.wait()
    lane = lax.broadcasted_iota(jnp.int32, (rows, lanes), 1)
    row = lax.broadcasted_iota(jnp.int32, (rows, lanes), 0)

    def apply(x, read, write):
        b = [[block[v, u, x] for u in range(variables)] for v in range(variables)]
        for n in range(count):
            src = [read(n, u) for u in range(variables)]
            for v in range(variables):
                total = b[v][0] * src[0]
                for u in range(1, variables):
                    total = total + b[v][u] * src[u]
                write(n, v, total)

    def keep(s, x):
        def write(n, v, value):
            update[s, n, v, x + 1] = value
            edge[s, 0, v, x, n:n + 1] = value[rows - 1:rows]
            edge[s, 1, v, x, n:n + 1] = value[0:1]
        return write

    def finish(x):
        def write(n, v, value):
            final[n, v, x] = state_blk[n, v, x] + value
        return write

    def first_plane(x):
        for v in range(variables):
            coupled = spectral_rows([state_blk[n, v, x] for n in range(count)])
            for n in range(count):
                residual[n, v, x] = -(part_blk[n, v, x] + coupled[n])
        apply(x, lambda n, u: residual[n, u, x], keep(0, x))

    def sweep_plane(s, x, writer):
        w = weight[x, row_block(me)]
        for v in range(variables):
            values = [update[s, n, v, x + 1] for n in range(count)]
            coupled = spectral_rows(values)
            for n in range(count):
                cur = values[n]
                beside = update[s, n, v, x] + update[s, n, v, x + 2] + lane_sum(cur, lane)
                over = pltpu.roll(cur, 1, 0)
                under = pltpu.roll(cur, rows - 1, 0)
                beside = beside + jnp.where(row == 0, halo[s, 0, v, x, n:n + 1], over)
                beside = beside + jnp.where(row == rows - 1, halo[s, 1, v, x, n:n + 1], under)
                source[n, v] = residual[n, v, x] - coupled[n] + w * beside
        apply(x, lambda n, u: source[n, u], writer)

    sent_x, sent_rows = [], []

    def start_planes(s):
        back = remote(update.at[s, :, :, 1], update.at[s, :, :, planes + 1],
                      send_u.at[s, 0], recv_u.at[s, 1], before)
        on = remote(update.at[s, :, :, planes], update.at[s, :, :, 0],
                    send_u.at[s, 1], recv_u.at[s, 0], after)
        pl.when(has_before)(back.start)
        pl.when(has_after)(on.start)
        sent_x.append((back, on))

    def start_rows(s):
        down = remote(edge.at[s, 0], halo.at[s, 0], send_r.at[s, 0], recv_r.at[s, 0], below)
        up = remote(edge.at[s, 1], halo.at[s, 1], send_r.at[s, 1], recv_r.at[s, 1], above)
        pl.when(has_below)(down.start)
        pl.when(has_above)(up.start)
        sent_rows.append((down, up))

    for move in moves + parts[0] + parts[1]:
        move.wait_recv()
    pl.loop(0, 2)(lambda i: first_plane(i * (planes - 1)))
    start_planes(0)
    for move in parts[2]:
        move.wait_recv()
    pl.loop(1, planes - 1)(first_plane)
    start_rows(0)

    returns = []

    def start_return(c, first, size):
        for step in range(1, inst_size):
            returns.append(remote(
                final.at[pl.ds(peer(step) * own, own), :, pl.ds(first, size)],
                out.at[:, :, pl.ds(first, size), row_block(me)],
                send_o.at[c, step], recv_o.at[c, step], {"inst": peer(step)}))
            returns[-1].start()

    half = planes // 2
    for s in range(SWEEPS):
        last = s == SWEEPS - 1
        down, up = sent_rows[s]
        pl.when(has_above)(down.wait_recv)
        pl.when(has_below)(up.wait_recv)

        def one(x):
            sweep_plane(s, x, finish(x) if last else keep(s + 1, x))

        if last:
            pl.loop(1, half)(one)
            start_return(0, 1, half - 1)
            pl.loop(half, planes - 1)(one)
            start_return(1, half, planes - 1 - half)
        else:
            pl.loop(1, planes - 1)(one)
        back, on = sent_x[s]
        pl.when(has_before)(on.wait_recv)
        pl.when(has_after)(back.wait_recv)
        pl.loop(0, 2)(lambda i: one(i * (planes - 1)))
        if last:
            start_return(2, 0, 1)
            start_return(3, planes - 1, 1)
        else:
            start_planes(s + 1)
            start_rows(s + 1)

    own_out = pltpu.make_async_copy(
        final.at[pl.ds(me * own, own)], out.at[:, :, :, row_block(me)], own_sem.at[1])
    own_out.start()
    for move in moves + parts[0] + parts[1] + parts[2]:
        move.wait_send()
    for back, on in [(to_before, to_after)] + sent_x:
        pl.when(has_before)(back.wait_send)
        pl.when(has_after)(on.wait_send)
    for down, up in sent_rows:
        pl.when(has_below)(down.wait_send)
        pl.when(has_above)(up.wait_send)
    own_out.wait()
    for move in returns:
        move.wait()


def on_device(flow_state, forcing, diffusion, block_inverse):
    inst_size, cells_size = lax.axis_size("inst"), lax.axis_size("cells")
    own, variables, planes, height, lanes = flow_state.shape
    count, rows = own * inst_size, height // inst_size
    f32 = jnp.float32
    dma = pltpu.SemaphoreType.DMA
    block_field = (count, variables, planes, rows, lanes)
    scratch = [
        pltpu.VMEM((own, variables, planes + 2, height, lanes), f32),
        pltpu.VMEM(forcing.shape, f32),
        pltpu.VMEM(diffusion.shape, f32),
        pltpu.VMEM(block_inverse.shape, f32),
        pltpu.VMEM(flow_state.shape, f32),
        pltpu.VMEM(block_field, f32),
        pltpu.VMEM(block_field, f32),
        pltpu.VMEM(block_field, f32),
        pltpu.VMEM((count, variables, rows, lanes), f32),
        pltpu.VMEM((SWEEPS, count, variables, planes + 2, rows, lanes), f32),
        pltpu.VMEM((SWEEPS, 2, variables, planes, count, lanes), f32),
        pltpu.VMEM((SWEEPS, 2, variables, planes, count, lanes), f32),
        pltpu.VMEM(block_field, f32),
        dma((5,)), dma((2,)),
        dma((inst_size,)), dma((inst_size,)),
        dma((3, inst_size)), dma((3, inst_size)),
        dma((2,)), dma((2,)),
        dma((SWEEPS, 2)), dma((SWEEPS, 2)),
        dma((SWEEPS, 2)), dma((SWEEPS, 2)),
        dma((4, inst_size)), dma((4, inst_size)),
    ]
    return pl.pallas_call(
        functools.partial(kernel, inst_size, cells_size),
        out_shape=jax.ShapeDtypeStruct(flow_state.shape, f32),
        in_specs=[pl.BlockSpec(memory_space=pl.ANY)] * 4,
        out_specs=pl.BlockSpec(memory_space=pl.ANY),
        scratch_shapes=scratch,
        compiler_params=pltpu.CompilerParams(collective_id=0, has_side_effects=True),
    )(flow_state, forcing, diffusion, block_inverse)


def solution(mesh):
    in_specs = (
        P("inst", None, "cells", None, None),
        P("inst", None, "cells", None, None),
        P("cells", None, None),
        P(None, None, "cells", "inst", None),
    )
    out_specs = P("inst", None, "cells", None, None)
    return jax.shard_map(
        on_device, mesh=mesh, in_specs=in_specs, out_specs=out_specs, check_vma=False
    )
```

```python
import functools
import math

import jax
import jax.numpy as jnp
from jax import lax
from jax.experimental import pallas as pl
from jax.experimental.pallas import tpu as pltpu
from jax.sharding import PartitionSpec as P

SWEEPS = 4

frequency = 1.0

MESH = pl.DeviceIdType.MESH


def spectral_rows(values):
    count = len(values)
    differences, products = {}, {}

    def product(coefficient, low, high):
        if (low, high) not in differences:
            differences[low, high] = values[low] - values[high]
        if (coefficient, low, high) not in products:
            products[coefficient, low, high] = coefficient * differences[low, high]
        return products[coefficient, low, high]

    rows = []
    for n in range(count):
        total = None
        for k in range(1, (count + 1) // 2):
            coefficient = frequency * 0.5 * (-1.0) ** k / math.tan(math.pi * k / count)
            a, b = (n - k) % count, (n + k) % count
            if a > b:
                a, b, coefficient = b, a, -coefficient
            if coefficient < 0:
                term, sign = product(-coefficient, a, b), -1
            else:
                term, sign = product(coefficient, a, b), 1
            if total is None:
                total = term if sign > 0 else -term
            else:
                total = total + term if sign > 0 else total - term
        rows.append(total)
    return rows


def lane_sum(cur, lane):
    size = cur.shape[-1]
    left = jnp.where(lane == 0, 0.0, pltpu.roll(cur, 1, 1))
    right = jnp.where(lane == size - 1, 0.0, pltpu.roll(cur, size - 1, 1))
    return left + right


def kernel(inst_size, cells_size, state, forcing, diffusion, blocks, out,
           home, force, weight, block, part, state_blk, part_blk, residual, source, update,
           edge, halo, final, load_sem, own_sem, send_a, recv_a, send_b, recv_b, send_x, recv_x,
           send_u, recv_u, send_r, recv_r, send_o, recv_o):
    me, cell = lax.axis_index("inst"), lax.axis_index("cells")
    own, variables, planes, height, lanes = state.shape
    rows = height // inst_size
    count = own * inst_size

    def peer(step):
        return lax.rem(me + step, inst_size)

    def row_block(i):
        return pl.ds(pl.multiple_of(i * rows, rows), rows)

    has_before, has_after = cell > 0, cell < cells_size - 1
    has_above, has_below = me > 0, me < inst_size - 1
    before, after = {"cells": cell - 1}, {"cells": cell + 1}
    above, below = {"inst": me - 1}, {"inst": me + 1}

    def remote(src, dst, send, recv, target):
        return pltpu.make_async_remote_copy(
            src_ref=src, dst_ref=dst, send_sem=send, recv_sem=recv,
            device_id=target, device_id_type=MESH)

    loads = [
        pltpu.make_async_copy(state, home.at[:, :, pl.ds(1, planes)], load_sem.at[0]),
        pltpu.make_async_copy(forcing, force, load_sem.at[1]),
        pltpu.make_async_copy(diffusion, weight, load_sem.at[2]),
        pltpu.make_async_copy(
            state.at[:, :, :, row_block(me)], state_blk.at[pl.ds(me * own, own)], load_sem.at[3]),
        pltpu.make_async_copy(blocks, block, load_sem.at[4]),
    ]
    for load in loads:
        load.start()

    zero_home = jnp.zeros((own, variables, height, lanes), jnp.float32)

    @pl.when(jnp.logical_not(has_before))
    def _():
        home[:, :, 0] = zero_home

    @pl.when(jnp.logical_not(has_after))
    def _():
        home[:, :, planes + 1] = zero_home

    for s in range(SWEEPS):
        zero_blk = jnp.zeros((count, variables, rows, lanes), jnp.float32)

        @pl.when(jnp.logical_not(has_before))
        def _():
            update[s, :, :, 0] = zero_blk

        @pl.when(jnp.logical_not(has_after))
        def _():
            update[s, :, :, planes + 1] = zero_blk

        zero_halo = jnp.zeros((variables, planes, count, lanes), jnp.float32)

        @pl.when(jnp.logical_not(has_above))
        def _():
            halo[s, 0] = zero_halo

        @pl.when(jnp.logical_not(has_below))
        def _():
            halo[s, 1] = zero_halo

    barrier = pltpu.get_barrier_semaphore()
    for step in range(1, inst_size):
        pl.semaphore_signal(barrier, 1, device_id={"inst": peer(step)}, device_id_type=MESH)

    @pl.when(has_before)
    def _():
        pl.semaphore_signal(barrier, 1, device_id=before, device_id_type=MESH)

    @pl.when(has_after)
    def _():
        pl.semaphore_signal(barrier, 1, device_id=after, device_id_type=MESH)

    ends = jnp.where(has_before, 1, 0) + jnp.where(has_after, 1, 0)
    pl.semaphore_wait(barrier, inst_size - 1 + ends)

    to_before = remote(state.at[:, :, 0], home.at[:, :, planes + 1],
                       send_x.at[0], recv_x.at[1], before)
    to_after = remote(state.at[:, :, planes - 1], home.at[:, :, 0],
                      send_x.at[1], recv_x.at[0], after)
    pl.when(has_before)(to_before.start)
    pl.when(has_after)(to_after.start)

    moves = []
    for step in range(1, inst_size):
        moves.append(remote(
            state.at[:, :, :, row_block(peer(step))], state_blk.at[pl.ds(me * own, own)],
            send_a.at[step], recv_a.at[step], {"inst": peer(step)}))
        moves[-1].start()

    for load in loads[:3]:
        load.wait()
    lane = lax.broadcasted_iota(jnp.int32, (height, lanes), 1)
    row = lax.broadcasted_iota(jnp.int32, (height, lanes), 0)

    def local_plane(x, p):
        w = weight[x]
        for n in range(own):
            for v in range(variables):
                cur = home[n, v, x + 1]
                beside = home[n, v, x] + home[n, v, x + 2] + lane_sum(cur, lane)
                beside = beside + jnp.where(row == 0, 0.0, pltpu.roll(cur, 1, 0))
                beside = beside + jnp.where(row == height - 1, 0.0, pltpu.roll(cur, height - 1, 0))
                part[n, v, p] = w * (6.0 * cur - beside) - force[n, v, x]

    half = planes // 2

    def outermost(one):
        pl.loop(0, 2)(lambda i: one(i * (planes - 1), i))

    def second(one):
        pl.loop(0, 2)(lambda i: one(1 + i * (planes - 3), 2 + i))

    def inner(first, end, one):
        pl.loop(first, end)(lambda x: one(x, x + 2))

    second(local_plane)
    inner(2, planes - 2, local_plane)

    @pl.when(has_before)
    def _():
        to_after.wait_recv()

    @pl.when(has_after)
    def _():
        to_before.wait_recv()

    outermost(local_plane)

    own_parts = pltpu.make_async_copy(
        part.at[:, :, :, row_block(me)], part_blk.at[pl.ds(me * own, own)], own_sem.at[0])
    own_parts.start()
    ends_of = (0, 2, 4, half + 2, planes)
    parts = [[] for _ in ends_of[1:]]

    def start_part(c):
        positions = pl.ds(ends_of[c], ends_of[c + 1] - ends_of[c])
        for step in range(1, inst_size):
            parts[c].append(remote(
                part.at[:, :, positions, row_block(peer(step))],
                part_blk.at[pl.ds(me * own, own), :, positions],
                send_b.at[c, step], recv_b.at[c, step], {"inst": peer(step)}))
            parts[c][-1].start()

    for c in range(3):
        start_part(c)
    loads[3].wait()
    loads[4].wait()
    own_parts.wait()
    lane = lax.broadcasted_iota(jnp.int32, (rows, lanes), 1)
    row = lax.broadcasted_iota(jnp.int32, (rows, lanes), 0)

    def apply(x, read, write):
        b = [[block[v, u, x] for u in range(variables)] for v in range(variables)]
        for n in range(count):
            src = [read(n, u) for u in range(variables)]
            for v in range(variables):
                total = b[v][0] * src[0]
                for u in range(1, variables):
                    total = total + b[v][u] * src[u]
                write(n, v, total)

    def keep(s, x, p):
        def write(n, v, value):
            update[s, n, v, x + 1] = value
            edge[s, 0, v, p, n:n + 1] = value[rows - 1:rows]
            edge[s, 1, v, p, n:n + 1] = value[0:1]
        return write

    def finish(x):
        def write(n, v, value):
            final[n, v, x] = state_blk[n, v, x] + value
        return write

    def first_plane(x, p):
        for v in range(variables):
            coupled = spectral_rows([state_blk[n, v, x] for n in range(count)])
            for n in range(count):
                residual[n, v, x] = -(part_blk[n, v, p] + coupled[n])
        apply(x, lambda n, u: residual[n, u, x], keep(0, x, p))

    def sweep_plane(s, x, p, writer):
        w = weight[x, row_block(me)]
        for v in range(variables):
            values = [update[s, n, v, x + 1] for n in range(count)]
            coupled = spectral_rows(values)
            for n in range(count):
                cur = values[n]
                beside = update[s, n, v, x] + update[s, n, v, x + 2] + lane_sum(cur, lane)
                over = pltpu.roll(cur, 1, 0)
                under = pltpu.roll(cur, rows - 1, 0)
                beside = beside + jnp.where(row == 0, halo[s, 0, v, p, n:n + 1], over)
                beside = beside + jnp.where(row == rows - 1, halo[s, 1, v, p, n:n + 1], under)
                source[n, v] = residual[n, v, x] - coupled[n] + w * beside
        apply(x, lambda n, u: source[n, u], writer)

    sent_x, sent_rows = [], {}

    def start_planes(s):
        back = remote(update.at[s, :, :, 1], update.at[s, :, :, planes + 1],
                      send_u.at[s, 0], recv_u.at[s, 1], before)
        on = remote(update.at[s, :, :, planes], update.at[s, :, :, 0],
                    send_u.at[s, 1], recv_u.at[s, 0], after)
        pl.when(has_before)(back.start)
        pl.when(has_after)(on.start)
        sent_x.append((back, on))

    def wait_planes(s):
        back, on = sent_x[s]
        pl.when(has_before)(on.wait_recv)
        pl.when(has_after)(back.wait_recv)

    def start_rows(s, g):
        positions = pl.ds(0, 2) if g == 0 else pl.ds(2, planes - 2)
        down = remote(edge.at[s, 0, :, positions], halo.at[s, 0, :, positions],
                      send_r.at[s, g, 0], recv_r.at[s, g, 0], below)
        up = remote(edge.at[s, 1, :, positions], halo.at[s, 1, :, positions],
                    send_r.at[s, g, 1], recv_r.at[s, g, 1], above)
        pl.when(has_below)(down.start)
        pl.when(has_above)(up.start)
        sent_rows[s, g] = (down, up)

    def wait_rows(s, g):
        down, up = sent_rows[s, g]
        pl.when(has_above)(down.wait_recv)
        pl.when(has_below)(up.wait_recv)

    def wait_part(c):
        for move in parts[c]:
            move.wait_recv()

    def swept(s):
        return lambda x, p: sweep_plane(s, x, p, keep(s + 1, x, p))

    def sweep_outermost(s):
        wait_planes(s)
        wait_rows(s, 0)
        outermost(swept(s))
        start_planes(s + 1)
        start_rows(s + 1, 0)

    def sweep_others(s):
        wait_rows(s, 1)
        second(swept(s))
        inner(2, planes - 2, swept(s))
        start_rows(s + 1, 1)

    for move in moves:
        move.wait_recv()
    wait_part(0)
    outermost(first_plane)
    start_planes(0)
    start_rows(0, 0)
    start_part(3)
    wait_part(1)
    second(first_plane)
    wait_part(2)
    inner(2, half, first_plane)
    sweep_outermost(0)
    wait_part(3)
    inner(half, planes - 2, first_plane)
    start_rows(0, 1)
    sweep_others(0)
    for s in range(1, SWEEPS - 1):
        if s < SWEEPS - 2:
            sweep_outermost(s)
            sweep_others(s)
        else:
            sweep_others(s)
            sweep_outermost(s)

    returns = []

    def start_return(c, first, size):
        for step in range(1, inst_size):
            returns.append(remote(
                final.at[pl.ds(peer(step) * own, own), :, pl.ds(first, size)],
                out.at[:, :, pl.ds(first, size), row_block(me)],
                send_o.at[c, step], recv_o.at[c, step], {"inst": peer(step)}))
            returns[-1].start()

    s = SWEEPS - 1

    def last(x, p):
        sweep_plane(s, x, p, finish(x))

    wait_rows(s, 1)
    inner(2, half, last)
    start_return(0, 2, half - 2)
    inner(half, planes - 2, last)
    start_return(1, half, planes - 2 - half)
    second(last)
    start_return(2, 1, 1)
    start_return(3, planes - 2, 1)
    wait_planes(s)
    wait_rows(s, 0)
    outermost(last)
    start_return(4, 0, 1)
    start_return(5, planes - 1, 1)

    own_out = pltpu.make_async_copy(
        final.at[pl.ds(me * own, own)], out.at[:, :, :, row_block(me)], own_sem.at[1])
    own_out.start()
    for move in moves + sum(parts, []):
        move.wait_send()
    for back, on in [(to_before, to_after)] + sent_x:
        pl.when(has_before)(back.wait_send)
        pl.when(has_after)(on.wait_send)
    for down, up in sent_rows.values():
        pl.when(has_below)(down.wait_send)
        pl.when(has_above)(up.wait_send)
    own_out.wait()
    for move in returns:
        move.wait()


def on_device(flow_state, forcing, diffusion, block_inverse):
    inst_size, cells_size = lax.axis_size("inst"), lax.axis_size("cells")
    own, variables, planes, height, lanes = flow_state.shape
    count, rows = own * inst_size, height // inst_size
    f32 = jnp.float32
    dma = pltpu.SemaphoreType.DMA
    block_field = (count, variables, planes, rows, lanes)
    scratch = [
        pltpu.VMEM((own, variables, planes + 2, height, lanes), f32),
        pltpu.VMEM(forcing.shape, f32),
        pltpu.VMEM(diffusion.shape, f32),
        pltpu.VMEM(block_inverse.shape, f32),
        pltpu.VMEM(flow_state.shape, f32),
        pltpu.VMEM(block_field, f32),
        pltpu.VMEM(block_field, f32),
        pltpu.VMEM(block_field, f32),
        pltpu.VMEM((count, variables, rows, lanes), f32),
        pltpu.VMEM((SWEEPS, count, variables, planes + 2, rows, lanes), f32),
        pltpu.VMEM((SWEEPS, 2, variables, planes, count, lanes), f32),
        pltpu.VMEM((SWEEPS, 2, variables, planes, count, lanes), f32),
        pltpu.VMEM(block_field, f32),
        dma((5,)), dma((2,)),
        dma((inst_size,)), dma((inst_size,)),
        dma((4, inst_size)), dma((4, inst_size)),
        dma((2,)), dma((2,)),
        dma((SWEEPS, 2)), dma((SWEEPS, 2)),
        dma((SWEEPS, 2, 2)), dma((SWEEPS, 2, 2)),
        dma((6, inst_size)), dma((6, inst_size)),
    ]
    return pl.pallas_call(
        functools.partial(kernel, inst_size, cells_size),
        out_shape=jax.ShapeDtypeStruct(flow_state.shape, f32),
        in_specs=[pl.BlockSpec(memory_space=pl.ANY)] * 4,
        out_specs=pl.BlockSpec(memory_space=pl.ANY),
        scratch_shapes=scratch,
        compiler_params=pltpu.CompilerParams(collective_id=0, has_side_effects=True),
    )(flow_state, forcing, diffusion, block_inverse)


def solution(mesh):
    in_specs = (
        P("inst", None, "cells", None, None),
        P("inst", None, "cells", None, None),
        P("cells", None, None),
        P(None, None, "cells", "inst", None),
    )
    out_specs = P("inst", None, "cells", None, None)
    return jax.shard_map(
        on_device, mesh=mesh, in_specs=in_specs, out_specs=out_specs, check_vma=False
    )
```

```python
import functools
import math

import jax
import jax.numpy as jnp
from jax import lax
from jax.experimental import pallas as pl
from jax.experimental.pallas import tpu as pltpu
from jax.sharding import PartitionSpec as P

SWEEPS = 4

frequency = 1.0

MESH = pl.DeviceIdType.MESH


def spectral_rows(values):
    count = len(values)
    differences, products = {}, {}

    def product(coefficient, low, high):
        if (low, high) not in differences:
            differences[low, high] = values[low] - values[high]
        if (coefficient, low, high) not in products:
            products[coefficient, low, high] = coefficient * differences[low, high]
        return products[coefficient, low, high]

    rows = []
    for n in range(count):
        total = None
        for k in range(1, (count + 1) // 2):
            coefficient = frequency * 0.5 * (-1.0) ** k / math.tan(math.pi * k / count)
            a, b = (n - k) % count, (n + k) % count
            if a > b:
                a, b, coefficient = b, a, -coefficient
            if coefficient < 0:
                term, sign = product(-coefficient, a, b), -1
            else:
                term, sign = product(coefficient, a, b), 1
            if total is None:
                total = term if sign > 0 else -term
            else:
                total = total + term if sign > 0 else total - term
        rows.append(total)
    return rows


def lane_sum(cur, lane):
    size = cur.shape[-1]
    left = jnp.where(lane == 0, 0.0, pltpu.roll(cur, 1, 1))
    right = jnp.where(lane == size - 1, 0.0, pltpu.roll(cur, size - 1, 1))
    return left + right


def kernel(inst_size, cells_size, state, forcing, diffusion, blocks, out,
           home, force, weight, block, part, state_blk, part_blk, residual, source, update,
           edge, halo, final, load_sem, own_sem, send_a, recv_a, send_b, recv_b, send_x, recv_x,
           send_u, recv_u, send_r, recv_r, send_o, recv_o):
    me, cell = lax.axis_index("inst"), lax.axis_index("cells")
    own, variables, planes, height, lanes = state.shape
    rows = height // inst_size
    count = own * inst_size

    def peer(step):
        return lax.rem(me + step, inst_size)

    def row_block(i):
        return pl.ds(pl.multiple_of(i * rows, rows), rows)

    has_before, has_after = cell > 0, cell < cells_size - 1
    has_above, has_below = me > 0, me < inst_size - 1
    before, after = {"cells": cell - 1}, {"cells": cell + 1}
    above, below = {"inst": me - 1}, {"inst": me + 1}

    def remote(src, dst, send, recv, target):
        return pltpu.make_async_remote_copy(
            src_ref=src, dst_ref=dst, send_sem=send, recv_sem=recv,
            device_id=target, device_id_type=MESH)

    loads = [
        pltpu.make_async_copy(state, home.at[:, :, pl.ds(1, planes)], load_sem.at[0]),
        pltpu.make_async_copy(forcing, force, load_sem.at[1]),
        pltpu.make_async_copy(diffusion, weight, load_sem.at[2]),
        pltpu.make_async_copy(
            state.at[:, :, :, row_block(me)], state_blk.at[pl.ds(me * own, own)], load_sem.at[3]),
        pltpu.make_async_copy(blocks, block, load_sem.at[4]),
    ]
    for load in loads:
        load.start()

    zero_home = jnp.zeros((own, variables, height, lanes), jnp.float32)

    @pl.when(jnp.logical_not(has_before))
    def _():
        home[:, :, 0] = zero_home

    @pl.when(jnp.logical_not(has_after))
    def _():
        home[:, :, planes + 1] = zero_home

    for s in range(SWEEPS):
        zero_blk = jnp.zeros((count, variables, rows, lanes), jnp.float32)

        @pl.when(jnp.logical_not(has_before))
        def _():
            update[s, :, :, 0] = zero_blk

        @pl.when(jnp.logical_not(has_after))
        def _():
            update[s, :, :, planes + 1] = zero_blk

        zero_halo = jnp.zeros((variables, planes, count, lanes), jnp.float32)

        @pl.when(jnp.logical_not(has_above))
        def _():
            halo[s, 0] = zero_halo

        @pl.when(jnp.logical_not(has_below))
        def _():
            halo[s, 1] = zero_halo

    barrier = pltpu.get_barrier_semaphore()
    for step in range(1, inst_size):
        pl.semaphore_signal(barrier, 1, device_id={"inst": peer(step)}, device_id_type=MESH)

    @pl.when(has_before)
    def _():
        pl.semaphore_signal(barrier, 1, device_id=before, device_id_type=MESH)

    @pl.when(has_after)
    def _():
        pl.semaphore_signal(barrier, 1, device_id=after, device_id_type=MESH)

    ends = jnp.where(has_before, 1, 0) + jnp.where(has_after, 1, 0)
    pl.semaphore_wait(barrier, inst_size - 1 + ends)

    to_before = remote(state.at[:, :, 0], home.at[:, :, planes + 1],
                       send_x.at[0], recv_x.at[1], before)
    to_after = remote(state.at[:, :, planes - 1], home.at[:, :, 0],
                      send_x.at[1], recv_x.at[0], after)
    pl.when(has_before)(to_before.start)
    pl.when(has_after)(to_after.start)

    half = planes // 2
    pieces = ((0, half), (planes - 2, 2), (half, planes - 2 - half))
    moves = [[] for _ in pieces]

    def start_state(c):
        first, size = pieces[c]
        for step in range(1, inst_size):
            moves[c].append(remote(
                state.at[:, :, pl.ds(first, size), row_block(peer(step))],
                state_blk.at[pl.ds(me * own, own), :, pl.ds(first, size)],
                send_a.at[c, step], recv_a.at[c, step], {"inst": peer(step)}))
            moves[c][-1].start()

    start_state(0)
    start_state(1)

    for load in loads[:3]:
        load.wait()
    lane = lax.broadcasted_iota(jnp.int32, (height, lanes), 1)
    row = lax.broadcasted_iota(jnp.int32, (height, lanes), 0)

    def local_plane(x, p, q):
        w = weight[x]
        for n in range(own):
            for v in range(variables):
                cur = home[n, v, x + 1]
                beside = home[n, v, x] + home[n, v, x + 2] + lane_sum(cur, lane)
                beside = beside + jnp.where(row == 0, 0.0, pltpu.roll(cur, 1, 0))
                beside = beside + jnp.where(row == height - 1, 0.0, pltpu.roll(cur, height - 1, 0))
                part[n, v, p] = w * (6.0 * cur - beside) - force[n, v, x]

    def outermost(one):
        pl.loop(0, 2)(lambda i: one(i * (planes - 1), i, i))

    def second(one):
        pl.loop(0, 2)(lambda i: one(1 + i * (planes - 3), 2 + i, 2 + i * (planes - 3)))

    def inner(first, end, one):
        pl.loop(first, end)(lambda x: one(x, x + 2, x + 1))

    second(local_plane)
    inner(2, planes - 2, local_plane)

    @pl.when(has_before)
    def _():
        to_after.wait_recv()

    @pl.when(has_after)
    def _():
        to_before.wait_recv()

    outermost(local_plane)

    own_parts = pltpu.make_async_copy(
        part.at[:, :, :, row_block(me)], part_blk.at[pl.ds(me * own, own)], own_sem.at[0])
    own_parts.start()
    ends_of = (0, 2, 4, half + 2, planes)
    parts = [[] for _ in ends_of[1:]]

    def start_part(c):
        positions = pl.ds(ends_of[c], ends_of[c + 1] - ends_of[c])
        for step in range(1, inst_size):
            parts[c].append(remote(
                part.at[:, :, positions, row_block(peer(step))],
                part_blk.at[pl.ds(me * own, own), :, positions],
                send_b.at[c, step], recv_b.at[c, step], {"inst": peer(step)}))
            parts[c][-1].start()

    start_part(0)
    start_state(2)
    start_part(1)
    start_part(2)
    loads[3].wait()
    loads[4].wait()
    own_parts.wait()
    lane = lax.broadcasted_iota(jnp.int32, (rows, lanes), 1)
    row = lax.broadcasted_iota(jnp.int32, (rows, lanes), 0)

    def apply(x, read, write):
        b = [[block[v, u, x] for u in range(variables)] for v in range(variables)]
        for n in range(count):
            src = [read(n, u) for u in range(variables)]
            for v in range(variables):
                total = b[v][0] * src[0]
                for u in range(1, variables):
                    total = total + b[v][u] * src[u]
                write(n, v, total)

    def keep(s, x, q):
        def write(n, v, value):
            update[s, n, v, x + 1] = value
            edge[s, 0, v, q, n:n + 1] = value[rows - 1:rows]
            edge[s, 1, v, q, n:n + 1] = value[0:1]
        return write

    def finish(x):
        def write(n, v, value):
            final[n, v, x] = state_blk[n, v, x] + value
        return write

    def first_plane(x, p, q):
        for v in range(variables):
            coupled = spectral_rows([state_blk[n, v, x] for n in range(count)])
            for n in range(count):
                residual[n, v, x] = -(part_blk[n, v, p] + coupled[n])
        apply(x, lambda n, u: residual[n, u, x], keep(0, x, q))

    def sweep_plane(s, x, q, writer):
        w = weight[x, row_block(me)]
        for v in range(variables):
            values = [update[s, n, v, x + 1] for n in range(count)]
            coupled = spectral_rows(values)
            for n in range(count):
                cur = values[n]
                beside = update[s, n, v, x] + update[s, n, v, x + 2] + lane_sum(cur, lane)
                over = pltpu.roll(cur, 1, 0)
                under = pltpu.roll(cur, rows - 1, 0)
                beside = beside + jnp.where(row == 0, halo[s, 0, v, q, n:n + 1], over)
                beside = beside + jnp.where(row == rows - 1, halo[s, 1, v, q, n:n + 1], under)
                source[n, v] = residual[n, v, x] - coupled[n] + w * beside
        apply(x, lambda n, u: source[n, u], writer)

    sent_x, sent_rows = [], {}

    def start_planes(s):
        back = remote(update.at[s, :, :, 1], update.at[s, :, :, planes + 1],
                      send_u.at[s, 0], recv_u.at[s, 1], before)
        on = remote(update.at[s, :, :, planes], update.at[s, :, :, 0],
                    send_u.at[s, 1], recv_u.at[s, 0], after)
        pl.when(has_before)(back.start)
        pl.when(has_after)(on.start)
        sent_x.append((back, on))

    def wait_planes(s):
        back, on = sent_x[s]
        pl.when(has_before)(on.wait_recv)
        pl.when(has_after)(back.wait_recv)

    row_ends = (0, 2, half + 1, planes)

    def start_rows(s, g):
        positions = pl.ds(row_ends[g], row_ends[g + 1] - row_ends[g])
        down = remote(edge.at[s, 0, :, positions], halo.at[s, 0, :, positions],
                      send_r.at[s, g, 0], recv_r.at[s, g, 0], below)
        up = remote(edge.at[s, 1, :, positions], halo.at[s, 1, :, positions],
                    send_r.at[s, g, 1], recv_r.at[s, g, 1], above)
        pl.when(has_below)(down.start)
        pl.when(has_above)(up.start)
        sent_rows[s, g] = (down, up)

    def wait_rows(s, g):
        down, up = sent_rows[s, g]
        pl.when(has_above)(down.wait_recv)
        pl.when(has_below)(up.wait_recv)

    def wait_part(c):
        for move in parts[c]:
            move.wait_recv()

    def wait_state(c):
        for move in moves[c]:
            move.wait_recv()

    def swept(s):
        return lambda x, p, q: sweep_plane(s, x, q, keep(s + 1, x, q))

    def sweep_outermost(s):
        wait_planes(s)
        wait_rows(s, 0)
        outermost(swept(s))
        start_planes(s + 1)
        start_rows(s + 1, 0)

    def sweep_others(s):
        wait_rows(s, 1)
        inner(1, half, swept(s))
        start_rows(s + 1, 1)
        wait_rows(s, 2)
        inner(half, planes - 1, swept(s))
        start_rows(s + 1, 2)

    wait_state(0)
    wait_state(1)
    wait_part(0)
    outermost(first_plane)
    start_planes(0)
    start_rows(0, 0)
    start_part(3)
    wait_part(1)
    second(first_plane)
    wait_part(2)
    inner(2, half, first_plane)
    start_rows(0, 1)
    sweep_outermost(0)
    wait_state(2)
    wait_part(3)
    inner(half, planes - 2, first_plane)
    start_rows(0, 2)
    sweep_others(0)
    for s in range(1, SWEEPS - 2):
        sweep_outermost(s)
        sweep_others(s)
    sweep_others(SWEEPS - 2)

    returns = []

    def start_return(c, first, size):
        for step in range(1, inst_size):
            returns.append(remote(
                final.at[pl.ds(peer(step) * own, own), :, pl.ds(first, size)],
                out.at[:, :, pl.ds(first, size), row_block(me)],
                send_o.at[c, step], recv_o.at[c, step], {"inst": peer(step)}))
            returns[-1].start()

    s = SWEEPS - 1

    def last(x, p, q):
        sweep_plane(s, x, q, finish(x))

    wait_rows(s, 1)
    inner(2, half, last)
    start_return(0, 2, half - 2)
    wait_rows(s, 2)
    inner(half, planes - 2, last)
    start_return(1, half, planes - 2 - half)
    sweep_outermost(s - 1)
    second(last)
    start_return(2, 1, 1)
    start_return(3, planes - 2, 1)
    wait_planes(s)
    wait_rows(s, 0)
    outermost(last)
    start_return(4, 0, 1)
    start_return(5, planes - 1, 1)

    own_out = pltpu.make_async_copy(
        final.at[pl.ds(me * own, own)], out.at[:, :, :, row_block(me)], own_sem.at[1])
    own_out.start()
    for move in sum(moves + parts, []):
        move.wait_send()
    for back, on in [(to_before, to_after)] + sent_x:
        pl.when(has_before)(back.wait_send)
        pl.when(has_after)(on.wait_send)
    for down, up in sent_rows.values():
        pl.when(has_below)(down.wait_send)
        pl.when(has_above)(up.wait_send)
    own_out.wait()
    for move in returns:
        move.wait()


def on_device(flow_state, forcing, diffusion, block_inverse):
    inst_size, cells_size = lax.axis_size("inst"), lax.axis_size("cells")
    own, variables, planes, height, lanes = flow_state.shape
    count, rows = own * inst_size, height // inst_size
    f32 = jnp.float32
    dma = pltpu.SemaphoreType.DMA
    block_field = (count, variables, planes, rows, lanes)
    scratch = [
        pltpu.VMEM((own, variables, planes + 2, height, lanes), f32),
        pltpu.VMEM(forcing.shape, f32),
        pltpu.VMEM(diffusion.shape, f32),
        pltpu.VMEM(block_inverse.shape, f32),
        pltpu.VMEM(flow_state.shape, f32),
        pltpu.VMEM(block_field, f32),
        pltpu.VMEM(block_field, f32),
        pltpu.VMEM(block_field, f32),
        pltpu.VMEM((count, variables, rows, lanes), f32),
        pltpu.VMEM((SWEEPS, count, variables, planes + 2, rows, lanes), f32),
        pltpu.VMEM((SWEEPS, 2, variables, planes, count, lanes), f32),
        pltpu.VMEM((SWEEPS, 2, variables, planes, count, lanes), f32),
        pltpu.VMEM(block_field, f32),
        dma((5,)), dma((2,)),
        dma((3, inst_size)), dma((3, inst_size)),
        dma((4, inst_size)), dma((4, inst_size)),
        dma((2,)), dma((2,)),
        dma((SWEEPS, 2)), dma((SWEEPS, 2)),
        dma((SWEEPS, 3, 2)), dma((SWEEPS, 3, 2)),
        dma((6, inst_size)), dma((6, inst_size)),
    ]
    return pl.pallas_call(
        functools.partial(kernel, inst_size, cells_size),
        out_shape=jax.ShapeDtypeStruct(flow_state.shape, f32),
        in_specs=[pl.BlockSpec(memory_space=pl.ANY)] * 4,
        out_specs=pl.BlockSpec(memory_space=pl.ANY),
        scratch_shapes=scratch,
        compiler_params=pltpu.CompilerParams(collective_id=0, has_side_effects=True),
    )(flow_state, forcing, diffusion, block_inverse)


def solution(mesh):
    in_specs = (
        P("inst", None, "cells", None, None),
        P("inst", None, "cells", None, None),
        P("cells", None, None),
        P(None, None, "cells", "inst", None),
    )
    out_specs = P("inst", None, "cells", None, None)
    return jax.shard_map(
        on_device, mesh=mesh, in_specs=in_specs, out_specs=out_specs, check_vma=False
    )
```
